16 devices in a mesh: rep: 2 (over y, z), dp: 8 (over x, core).
Axes of the slice: x: 4, y: 2, z: 1, core: 2. Of those that a mesh axis runs over, the one named last changes fastest.
The devices are a block of a 4x4x8 slice.
Arguments:
- g_w_gate: bfloat16 [16, 2, 1024, 4096], P(('rep', 'dp')), parts along dimension 0
- g_w_up: bfloat16 [16, 2, 1024, 4096], P(('rep', 'dp')), parts along dimension 0
- g_w_down: bfloat16 [16, 2, 4096, 1024], P(('rep', 'dp')), parts along dimension 0
- w_gate: bfloat16 [2, 1024, 4096], replicated
- w_up: bfloat16 [2, 1024, 4096], replicated
- w_down: bfloat16 [2, 4096, 1024], replicated
- m_w_gate: float32 [2, 1024, 4096], P(None, 'dp')
- m_w_up: float32 [2, 1024, 4096], P(None, 'dp')
- m_w_down: float32 [2, 4096, 1024], P(None, 'dp')
- v_w_gate: float32 [2, 1024, 4096], P(None, 'dp')
- v_w_up: float32 [2, 1024, 4096], P(None, 'dp')
- v_w_down: float32 [2, 4096, 1024], P(None, 'dp')
Outputs:
- output 1: bfloat16 [4, 1024, 4096], P('rep'), parts along dimension 0
- output 2: bfloat16 [4, 1024, 4096], P('rep'), parts along dimension 0
- output 3: bfloat16 [4, 4096, 1024], P('rep'), parts along dimension 0
- output 4: float32 [4, 1024, 4096], P('rep', 'dp'), parts along dimension 0
- output 5: float32 [4, 1024, 4096], P('rep', 'dp'), parts along dimension 0
- output 6: float32 [4, 4096, 1024], P('rep', 'dp'), parts along dimension 0
- output 7: float32 [4, 1024, 4096], P('rep', 'dp'), parts along dimension 0
- output 8: float32 [4, 1024, 4096], P('rep', 'dp'), parts along dimension 0
- output 9: float32 [4, 4096, 1024], P('rep', 'dp'), parts along dimension 0
There are 2 independent parts. The reference program is written for one: setup_inputs(seed, part) draws one part's arguments, and reference() takes and returns one part's arrays. A program takes and returns all parts, laid end to end along the dimension named above; an argument that names none is the same for every part.
All inputs are finite; a program needn't handle non-finite values.
Results may differ from the reference program's by a relative error of at most 0.022.
Values are sent between devices in bfloat16 or wider.
A program may use at most 768 MiB of HBM per device.

```python
import jax
import jax.numpy as jnp
from jax import lax

DEVICES = 8
D = 1024
FF = 4096
LAYERS = 2
NAMES = ("w_gate", "w_up", "w_down")
SHAPES = {"w_gate": (LAYERS, D, FF), "w_up": (LAYERS, D, FF), "w_down": (LAYERS, FF, D)}


def setup_inputs(seed: int = 0, part: int = 0) -> dict:
    kz, *keys = jax.random.split(jax.random.key(seed), 1 + 5 * len(NAMES))
    loud = 2.0 ** jax.random.uniform(kz, (), jnp.float32, -1.0, 1.0)
    drawn = {}
    for name, key, both in zip(NAMES, keys[:3], keys[3:6], strict=True):
        own = jax.random.normal(jax.random.fold_in(key, part), (DEVICES, *SHAPES[name]), jnp.float32)
        shared = jax.random.normal(jax.random.fold_in(both, part), SHAPES[name], jnp.float32)
        drawn["g_" + name] = (loud * (0.7 * shared / DEVICES + 0.7 * own * DEVICES**-0.5)).astype(jnp.bfloat16)
    for name, key in zip(NAMES, keys[6:9], strict=True):
        drawn[name] = (jax.random.normal(key, SHAPES[name], jnp.float32) * SHAPES[name][1] ** -0.5).astype(jnp.bfloat16)
    for name, key in zip(NAMES, keys[9:12], strict=True):
        drawn["m_" + name] = loud * 0.5 * jax.random.normal(key, SHAPES[name], jnp.float32)
    for name, key in zip(NAMES, keys[12:15], strict=True):
        drawn["v_" + name] = loud * loud * jax.random.uniform(key, SHAPES[name], jnp.float32, 0.5, 1.5)
    return drawn


def adamw(w, m, v, g):
    m = 0.9 * m + 0.1 * g
    v = 0.95 * v + 0.05 * g * g
    step = m * lax.rsqrt(v + 1e-8) + 0.1 * w
    return (w - 0.02 * step).astype(jnp.bfloat16), m, v


def reference(g_w_gate, g_w_up, g_w_down, w_gate, w_up, w_down, m_w_gate, m_w_up, m_w_down, v_w_gate, v_w_up, v_w_down):
    def total(terms):
        return lax.scan(lambda so_far, term: (so_far + term.astype(jnp.float32), None), jnp.zeros(terms.shape[1:], jnp.float32), terms)[0]

    gradients = [total(terms).astype(jnp.bfloat16).astype(jnp.float32) for terms in (g_w_gate, g_w_up, g_w_down)]
    new = [
        adamw(w.astype(jnp.float32), m, v, g)
        for w, m, v, g in zip((w_gate, w_up, w_down), (m_w_gate, m_w_up, m_w_down), (v_w_gate, v_w_up, v_w_down), gradients, strict=True)
    ]
    return tuple(one[which] for which in range(3) for one in new)
```

```python
import functools

import jax
import jax.numpy as jnp
from jax import lax
from jax.experimental import pallas as pl
from jax.experimental.pallas import tpu as pltpu
from jax.sharding import PartitionSpec as P

MESH = pl.DeviceIdType.MESH
ROWS, COLS = 128, 1024
HALF = ROWS // 2
SUB = 16
SLOTS = 4
CORES = 2
A, B = slice(0, HALF), slice(HALF, ROWS)


def adamw(w, m, v, g):
    m = 0.9 * m + 0.1 * g
    v = 0.95 * v + 0.05 * g * g
    step = m * lax.rsqrt(v + 1e-8) + 0.1 * w
    return (w - 0.02 * step).astype(jnp.bfloat16), m, v


def row_loop(first, rows, body):
    def step(i, carry):
        body(pl.ds(pl.multiple_of(first + i * SUB, SUB), SUB))
        return carry

    lax.fori_loop(0, rows // SUB, step, 0)


def kernel(axis, chips, per, units, *refs):
    g, w, m, v = (refs[i : i + 3] for i in (0, 3, 6, 9))
    out, m_out, v_out = (refs[i : i + 3] for i in (12, 15, 18))
    own, pair, arrived, hop, w_v, m_v, v_v = refs[21:28]
    (load_sem, store_sem, pair_sem, hop_sem, arrived_sem, left_sem, right_sem, far_sem, send_sem, gather_sem, tail_sem) = refs[28:]

    me = lax.axis_index(axis)
    chip, core = me // CORES, lax.rem(me, CORES)
    other = 1 - core
    right_chip, left_chip, far_chip = (lax.rem(chip + d, chips) for d in (1, chips - 1, 2))
    right, left, partner = right_chip * CORES + core, left_chip * CORES + core, chip * CORES + other

    def to(device):
        return {"device_id": {axis: device}, "device_id_type": MESH}

    def part(k, u):
        rest = u - k * per
        quarters = per // 2
        return rest // quarters, lax.rem(rest, quarters)

    def block(ref, k, u, who, which):
        layer, q = part(k, u)
        if k < 2:
            return ref.at[layer, who, which, :, pl.ds(pl.multiple_of(q * COLS, COLS), COLS)]
        return ref.at[layer, who, which, q]

    def moment(ref, k, u):
        layer, q = part(k, u)
        if k < 2:
            return ref.at[layer, :, pl.ds(pl.multiple_of(q * COLS, COLS), COLS)]
        return ref.at[layer, q]

    def each_weight(u, body):
        for k in range(3):
            pl.when((u >= k * per) & (u < (k + 1) * per))(functools.partial(body, k))

    def loads(k, u):
        slot = lax.rem(u, SLOTS)
        return (
            pltpu.make_async_copy(block(g[k], k, u, slice(None), core), own.at[slot], load_sem.at[slot, 0]),
            pltpu.make_async_copy(block(w[k], k, u, chip, core), w_v.at[slot], load_sem.at[slot, 1]),
            pltpu.make_async_copy(moment(m[k], k, u), m_v.at[slot], load_sem.at[slot, 2]),
            pltpu.make_async_copy(moment(v[k], k, u), v_v.at[slot], load_sem.at[slot, 3]),
        )

    def stores(k, u):
        slot = lax.rem(u, SLOTS)
        return (
            pltpu.make_async_copy(m_v.at[slot], moment(m_out[k], k, u), store_sem.at[slot, 0]),
            pltpu.make_async_copy(v_v.at[slot], moment(v_out[k], k, u), store_sem.at[slot, 1]),
        )

    def remote(src, dst, send, recv, device):
        return pltpu.make_async_remote_copy(src_ref=src, dst_ref=dst, send_sem=send, recv_sem=recv, **to(device))

    def load(u):
        def body(k):
            for copy in loads(k, u):
                copy.start()
            remote(block(g[k], k, u, slice(None), other), pair.at[u], send_sem.at[k], pair_sem.at[u], partner).start()

        each_weight(u, body)

    def first_hop(u):
        slot = lax.rem(u, SLOTS)
        pltpu.make_async_copy(own.at[slot], own.at[slot], load_sem.at[slot, 0]).wait()
        pltpu.make_async_copy(pair.at[u], pair.at[u], pair_sem.at[u]).wait()

        def add(who, first, rows):
            def body(r):
                pair[u, who, r, :] = (own[slot, who, r, :].astype(jnp.float32) + pair[u, who, r, :].astype(jnp.float32)).astype(jnp.bfloat16)

            row_loop(first, rows, body)

        add(far_chip, 0, ROWS)
        remote(pair.at[u, far_chip, A], hop.at[u, A], send_sem.at[3], hop_sem.at[u], right).start()
        remote(pair.at[u, far_chip, B], hop.at[u, B], send_sem.at[3], hop_sem.at[u], left).start()
        add(right_chip, HALF, HALF)
        remote(pair.at[u, right_chip, B], arrived.at[u, 0, B], send_sem.at[3], arrived_sem.at[u], right).start()
        add(left_chip, 0, HALF)
        remote(pair.at[u, left_chip, A], arrived.at[u, 1, A], send_sem.at[3], arrived_sem.at[u], left).start()

    def second_hop(u):
        slot = lax.rem(u, SLOTS)
        pltpu.make_async_copy(hop.at[u], hop.at[u], hop_sem.at[u]).wait()

        def add(who, first, rows):
            def body(r):
                total = own[slot, who, r, :].astype(jnp.float32) + pair[u, who, r, :].astype(jnp.float32)
                hop[u, r, :] = (total + hop[u, r, :].astype(jnp.float32)).astype(jnp.bfloat16)

            row_loop(first, rows, body)

        add(right_chip, 0, HALF)
        remote(hop.at[u, A], arrived.at[u, 0, A], send_sem.at[4], arrived_sem.at[u], right).start()
        add(left_chip, HALF, HALF)
        remote(hop.at[u, B], arrived.at[u, 1, B], send_sem.at[4], arrived_sem.at[u], left).start()

    def update(u):
        slot = lax.rem(u, SLOTS)
        pltpu.make_async_copy(arrived.at[u], arrived.at[u], arrived_sem.at[u]).wait()
        for i, ref in enumerate((w_v, m_v, v_v)):
            pltpu.make_async_copy(ref.at[slot], ref.at[slot], load_sem.at[slot, 1 + i]).wait()

        def body(r):
            total = own[slot, chip, r, :].astype(jnp.float32) + pair[u, chip, r, :].astype(jnp.float32)
            total = total + arrived[u, 0, r, :].astype(jnp.float32)
            total = total + arrived[u, 1, r, :].astype(jnp.float32)
            total = total.astype(jnp.bfloat16).astype(jnp.float32)
            new_w, new_m, new_v = adamw(w_v[slot, r, :].astype(jnp.float32), m_v[slot, r, :], v_v[slot, r, :], total)
            arrived[u, 0, r, :] = new_w
            m_v[slot, r, :] = new_m
            v_v[slot, r, :] = new_v

        row_loop(0, ROWS, body)

        def send(k):
            new, where = arrived.at[u, 0], block(out[k], k, u, chip, core)
            remote(new, where, send_sem.at[5], left_sem.at[u], right).start()
            remote(new, where, send_sem.at[6], right_sem.at[u], left).start()
            remote(new, where, send_sem.at[7], gather_sem.at[k], partner).start()
            pltpu.make_async_copy(new, where, tail_sem).start()
            for copy in stores(k, u):
                copy.start()

        each_weight(u, send)

    def stored(u):
        def body(k):
            for copy in stores(k, u):
                copy.wait()

        each_weight(u, body)

    def forward(u):
        def body(k):
            from_left, from_right = block(out[k], k, u, left_chip, core), block(out[k], k, u, right_chip, core)
            pltpu.make_async_copy(from_left, from_left, left_sem.at[u]).wait()
            remote(from_left.at[A], from_left.at[A], send_sem.at[8], far_sem.at[u], right).start()
            remote(from_left, from_left, send_sem.at[9], gather_sem.at[k], partner).start()
            pltpu.make_async_copy(from_right, from_right, right_sem.at[u]).wait()
            remote(from_right.at[B], from_right.at[B], send_sem.at[10], far_sem.at[u], left).start()
            remote(from_right, from_right, send_sem.at[11], gather_sem.at[k], partner).start()

        each_weight(u, body)

    def last(u):
        def body(k):
            from_far = block(out[k], k, u, far_chip, core)
            pltpu.make_async_copy(from_far, from_far, far_sem.at[u]).wait()
            remote(from_far, from_far, send_sem.at[12], gather_sem.at[k], partner).start()

        each_weight(u, body)

    barrier = pltpu.get_barrier_semaphore()
    for device in (left, right, partner):
        pl.semaphore_signal(barrier, inc=1, **to(device))
    pl.semaphore_wait(barrier, 3)

    load(0)

    def step(t, carry):
        @pl.when((t >= SLOTS - 1) & (t < units + SLOTS - 1))
        def _():
            stored(t - (SLOTS - 1))

        @pl.when(t < units - 1)
        def _():
            load(t + 1)

        for lag, stage in enumerate((first_hop, second_hop, update, forward, last)):
            pl.when((t >= lag) & (t < units + lag))(functools.partial(stage, t - lag))
        return carry

    lax.fori_loop(0, units + 4, step, 0)

    for k in range(3):
        sent = g[k].at[:, :, other]
        pltpu.make_async_copy(sent, sent, send_sem.at[k]).wait()
    for i, ref in ((3, arrived), (4, hop), (5, hop), (6, hop), (7, hop), (8, hop.at[:, A]), (9, hop), (10, hop.at[:, B]), (11, hop), (12, hop)):
        pltpu.make_async_copy(ref, ref, send_sem.at[i]).wait()
    for k in range(3):
        got = out[k].at[:, :, other]
        pltpu.make_async_copy(got, got, gather_sem.at[k]).wait()
    pltpu.make_async_copy(hop, hop, tail_sem).wait()


def solution(mesh):
    axis = "dp"
    chips = mesh.shape[axis] // CORES
    assert chips == 4

    def step(*arrays):
        def cut(x, rows, columns, split):
            lead = (x.shape[0],) + ((chips, CORES) if split else ())
            return x.reshape(*lead, *((rows, columns) if columns > COLS else (rows // ROWS, ROWS, columns)))

        shapes = [a.shape for a in arrays[6:9]]
        assert all(s[1] == ROWS for s in shapes[:2])
        per = shapes[0][0] * shapes[0][2] // COLS
        units = 3 * per
        g = [cut(a[0], s[1], s[2], True) for a, s in zip(arrays[:3], shapes, strict=True)]
        w = [cut(a, s[1], s[2], True) for a, s in zip(arrays[3:6], shapes, strict=True)]
        moments = [cut(a, s[1], s[2], False) for a, s in zip(arrays[6:], shapes + shapes, strict=True)]
        hbm = pl.BlockSpec(memory_space=pltpu.HBM)
        result = pl.pallas_call(
            functools.partial(kernel, axis, chips, per, units),
            out_shape=[jax.ShapeDtypeStruct(x.shape, x.dtype) for x in (*w, *moments)],
            in_specs=[hbm] * 12,
            out_specs=[hbm] * 9,
            scratch_shapes=[
                pltpu.VMEM((SLOTS, chips, ROWS, COLS), jnp.bfloat16),
                pltpu.VMEM((units, chips, ROWS, COLS), jnp.bfloat16),
                pltpu.VMEM((units, 2, ROWS, COLS), jnp.bfloat16),
                pltpu.VMEM((units, ROWS, COLS), jnp.bfloat16),
                pltpu.VMEM((SLOTS, ROWS, COLS), jnp.bfloat16),
                pltpu.VMEM((SLOTS, ROWS, COLS), jnp.float32),
                pltpu.VMEM((SLOTS, ROWS, COLS), jnp.float32),
                pltpu.SemaphoreType.DMA((SLOTS, 4)),
                pltpu.SemaphoreType.DMA((SLOTS, 2)),
                pltpu.SemaphoreType.DMA((units,)),
                pltpu.SemaphoreType.DMA((units,)),
                pltpu.SemaphoreType.DMA((units,)),
                pltpu.SemaphoreType.DMA((units,)),
                pltpu.SemaphoreType.DMA((units,)),
                pltpu.SemaphoreType.DMA((units,)),
                pltpu.SemaphoreType.DMA((13,)),
                pltpu.SemaphoreType.DMA((3,)),
                pltpu.SemaphoreType.DMA,
            ],
            compiler_params=pltpu.CompilerParams(collective_id=0, has_side_effects=True, vmem_limit_bytes=62 * 1024 * 1024),
        )(*g, *w, *moments)
        return tuple(x.reshape(a.shape) for x, a in zip(result, arrays[3:], strict=True))

    all_of, cut_of = P(None, None, None), P(None, "dp", None)
    return jax.shard_map(
        step,
        mesh=mesh,
        in_specs=(P(("rep", "dp"), None, None, None),) * 3 + (all_of,) * 3 + (cut_of,) * 6,
        out_specs=(P("rep", None, None),) * 3 + (P("rep", "dp", None),) * 6,
        check_vma=False,
    )
```

```python
import functools

import jax
import jax.numpy as jnp
from jax import lax
from jax.experimental import pallas as pl
from jax.experimental.pallas import tpu as pltpu
from jax.sharding import PartitionSpec as P

MESH = pl.DeviceIdType.MESH
ROWS, COLS = 128, 1024
HALF = ROWS // 2
SUB = 16
SLOTS = 4
CORES = 2
KEPT = 8
COPY_SLOTS, COPY_AHEAD = 12, 6
A, B = slice(0, HALF), slice(HALF, ROWS)


def adamw(w, m, v, g):
    m = 0.9 * m + 0.1 * g
    v = 0.95 * v + 0.05 * g * g
    step = m * lax.rsqrt(v + 1e-8) + 0.1 * w
    return (w - 0.02 * step).astype(jnp.bfloat16), m, v


def row_loop(first, rows, body):
    def step(i, carry):
        body(pl.ds(pl.multiple_of(first + i * SUB, SUB), SUB))
        return carry

    lax.fori_loop(0, rows // SUB, step, 0)


def kernel(axis, chips, per, units, kept, *refs):
    g, w, m, v = (refs[i : i + 3] for i in (0, 3, 6, 9))
    out, m_out, v_out = (refs[i : i + 3] for i in (12, 15, 18))
    to_right, to_left = refs[21:23]
    own, pair, arrived, hop, w_v, m_v, v_v = refs[23:30]
    (load_sem, store_sem, pair_sem, hop_sem, arrived_sem, left_sem, right_sem, far_sem, bounce_sem, send_sem, gather_sem, tail_sem) = refs[30:]

    me = lax.axis_index(axis)
    chip, core = me // CORES, lax.rem(me, CORES)
    other = 1 - core
    right_chip, left_chip, far_chip = (lax.rem(chip + d, chips) for d in (1, chips - 1, 2))
    right, left, partner = right_chip * CORES + core, left_chip * CORES + core, chip * CORES + other

    def to(device):
        return {"device_id": {axis: device}, "device_id_type": MESH}

    def part(k, u):
        rest = u - k * per
        quarters = per // 2
        return rest // quarters, lax.rem(rest, quarters)

    def block(ref, k, u, who, which):
        layer, q = part(k, u)
        if k < 2:
            return ref.at[layer, who, which, :, pl.ds(pl.multiple_of(q * COLS, COLS), COLS)]
        return ref.at[layer, who, which, q]

    def moment(ref, k, u):
        layer, q = part(k, u)
        if k < 2:
            return ref.at[layer, :, pl.ds(pl.multiple_of(q * COLS, COLS), COLS)]
        return ref.at[layer, q]

    def each_weight(u, body):
        for k in range(3):
            pl.when((u >= k * per) & (u < (k + 1) * per))(functools.partial(body, k))

    def loads(k, u):
        slot = lax.rem(u, SLOTS)
        return (
            pltpu.make_async_copy(block(g[k], k, u, slice(None), core), own.at[slot], load_sem.at[slot, 0]),
            pltpu.make_async_copy(block(w[k], k, u, chip, core), w_v.at[slot], load_sem.at[slot, 1]),
            pltpu.make_async_copy(moment(m[k], k, u), m_v.at[slot], load_sem.at[slot, 2]),
            pltpu.make_async_copy(moment(v[k], k, u), v_v.at[slot], load_sem.at[slot, 3]),
        )

    def stores(k, u):
        slot = lax.rem(u, SLOTS)
        return (
            pltpu.make_async_copy(m_v.at[slot], moment(m_out[k], k, u), store_sem.at[slot, 0]),
            pltpu.make_async_copy(v_v.at[slot], moment(v_out[k], k, u), store_sem.at[slot, 1]),
        )

    def remote(src, dst, send, recv, device):
        return pltpu.make_async_remote_copy(src_ref=src, dst_ref=dst, send_sem=send, recv_sem=recv, **to(device))

    def load(u):
        def body(k):
            for copy in loads(k, u):
                copy.start()
            remote(block(g[k], k, u, slice(None), other), pair.at[u], send_sem.at[k], pair_sem.at[u], partner).start()

        each_weight(u, body)

    def first_hop(u):
        slot = lax.rem(u, SLOTS)
        pltpu.make_async_copy(own.at[slot], own.at[slot], load_sem.at[slot, 0]).wait()
        pltpu.make_async_copy(pair.at[u], pair.at[u], pair_sem.at[u]).wait()

        def add(who, first, rows):
            def body(r):
                pair[u, who, r, :] = (own[slot, who, r, :].astype(jnp.float32) + pair[u, who, r, :].astype(jnp.float32)).astype(jnp.bfloat16)

            row_loop(first, rows, body)

        add(far_chip, 0, ROWS)
        remote(pair.at[u, far_chip, A], hop.at[u, A], send_sem.at[3], hop_sem.at[u], right).start()
        remote(pair.at[u, far_chip, B], hop.at[u, B], send_sem.at[3], hop_sem.at[u], left).start()
        add(right_chip, HALF, HALF)
        remote(pair.at[u, right_chip, B], arrived.at[u, 0, B], send_sem.at[3], arrived_sem.at[u], right).start()
        add(left_chip, 0, HALF)
        remote(pair.at[u, left_chip, A], arrived.at[u, 1, A], send_sem.at[3], arrived_sem.at[u], left).start()

    def second_hop(u):
        slot = lax.rem(u, SLOTS)
        pltpu.make_async_copy(hop.at[u], hop.at[u], hop_sem.at[u]).wait()

        def add(who, first, rows):
            def body(r):
                total = own[slot, who, r, :].astype(jnp.float32) + pair[u, who, r, :].astype(jnp.float32)
                hop[u, r, :] = (total + hop[u, r, :].astype(jnp.float32)).astype(jnp.bfloat16)

            row_loop(first, rows, body)

        add(right_chip, 0, HALF)
        remote(hop.at[u, A], arrived.at[u, 0, A], send_sem.at[4], arrived_sem.at[u], right).start()
        add(left_chip, HALF, HALF)
        remote(hop.at[u, B], arrived.at[u, 1, B], send_sem.at[4], arrived_sem.at[u], left).start()

    def update(u):
        slot = lax.rem(u, SLOTS)
        pltpu.make_async_copy(arrived.at[u], arrived.at[u], arrived_sem.at[u]).wait()
        for i, ref in enumerate((w_v, m_v, v_v)):
            pltpu.make_async_copy(ref.at[slot], ref.at[slot], load_sem.at[slot, 1 + i]).wait()

        def body(r):
            total = own[slot, chip, r, :].astype(jnp.float32) + pair[u, chip, r, :].astype(jnp.float32)
            total = total + arrived[u, 0, r, :].astype(jnp.float32)
            total = total + arrived[u, 1, r, :].astype(jnp.float32)
            total = total.astype(jnp.bfloat16).astype(jnp.float32)
            new_w, new_m, new_v = adamw(w_v[slot, r, :].astype(jnp.float32), m_v[slot, r, :], v_v[slot, r, :], total)
            arrived[u, 0, r, :] = new_w
            m_v[slot, r, :] = new_m
            v_v[slot, r, :] = new_v

        row_loop(0, ROWS, body)

        def send(k):
            new, where = arrived.at[u, 0], block(out[k], k, u, chip, core)
            remote(new, where, send_sem.at[5], left_sem.at[u], right).start()
            remote(new, where, send_sem.at[6], right_sem.at[u], left).start()
            remote(new, where, send_sem.at[7], gather_sem.at[k], partner).start()
            pltpu.make_async_copy(new, where, tail_sem).start()
            for copy in stores(k, u):
                copy.start()

        each_weight(u, send)

    def stored(u):
        def body(k):
            for copy in stores(k, u):
                copy.wait()

        each_weight(u, body)

    def bounces(k, u):
        slot = lax.rem(u, SLOTS)
        from_left, from_right = block(out[k], k, u, left_chip, core), block(out[k], k, u, right_chip, core)
        return (
            pltpu.make_async_copy(from_left.at[A], arrived.at[u, 1, A], bounce_sem.at[slot, 0]),
            pltpu.make_async_copy(from_right.at[B], arrived.at[u, 1, B], bounce_sem.at[slot, 1]),
        )

    def forward(u):
        def body(k):
            from_left, from_right = block(out[k], k, u, left_chip, core), block(out[k], k, u, right_chip, core)
            pltpu.make_async_copy(from_left, from_left, left_sem.at[u]).wait()

            @pl.when(u < kept)
            def _():
                remote(from_left.at[A], from_left.at[A], send_sem.at[8], far_sem.at[u], right).start()

            remote(from_left, from_left, send_sem.at[9], gather_sem.at[k], partner).start()
            pltpu.make_async_copy(from_right, from_right, right_sem.at[u]).wait()

            @pl.when(u < kept)
            def _():
                remote(from_right.at[B], from_right.at[B], send_sem.at[10], far_sem.at[u], left).start()

            remote(from_right, from_right, send_sem.at[11], gather_sem.at[k], partner).start()

            @pl.when(u >= kept)
            def _():
                for copy in bounces(k, u):
                    copy.start()

        each_weight(u, body)

    def last(u):
        def body(k):
            @pl.when(u < kept)
            def _():
                from_far = block(out[k], k, u, far_chip, core)
                pltpu.make_async_copy(from_far, from_far, far_sem.at[u]).wait()
                remote(from_far, from_far, send_sem.at[12], gather_sem.at[k], partner).start()

            @pl.when(u >= kept)
            def _():
                for copy in bounces(k, u):
                    copy.wait()
                pltpu.make_async_copy(arrived.at[u, 1, A], to_right.at[u - kept], bounce_sem.at[SLOTS, 0]).start()
                pltpu.make_async_copy(arrived.at[u, 1, B], to_left.at[u - kept], bounce_sem.at[SLOTS, 1]).start()

        each_weight(u, body)

    barrier = pltpu.get_barrier_semaphore()
    for device in (left, right, partner):
        pl.semaphore_signal(barrier, inc=1, **to(device))
    pl.semaphore_wait(barrier, 3)

    load(0)

    def step(t, carry):
        @pl.when((t >= SLOTS - 1) & (t < units + SLOTS - 1))
        def _():
            stored(t - (SLOTS - 1))

        @pl.when(t < units - 1)
        def _():
            load(t + 1)

        for lag, stage in enumerate((first_hop, second_hop, update, forward, last)):
            pl.when((t >= lag) & (t < units + lag))(functools.partial(stage, t - lag))
        return carry

    lax.fori_loop(0, units + 4, step, 0)

    for k in range(3):
        sent = g[k].at[:, :, other]
        pltpu.make_async_copy(sent, sent, send_sem.at[k]).wait()
    first = pl.ds(0, kept)
    for i, ref in ((3, arrived), (4, hop), (5, hop), (6, hop), (7, hop), (8, hop.at[first, A]), (9, hop), (10, hop.at[first, B]), (11, hop), (12, hop.at[first])):
        pltpu.make_async_copy(ref, ref, send_sem.at[i]).wait()
    for k in range(3):
        whole = min(max(kept - k * per, 0), per)
        got = arrived.at[pl.ds(0, (3 * per + whole) // 2)]
        pltpu.make_async_copy(got, got, gather_sem.at[k]).wait()
    pltpu.make_async_copy(hop, hop, tail_sem).wait()
    for i, ref in enumerate((to_right, to_left)):
        pltpu.make_async_copy(ref, ref, bounce_sem.at[SLOTS, i]).wait()


def copy_kernel(axis, chips, per, kept, *refs):
    sources, results, buffers, (in_sem, out_sem) = refs[:9], refs[9:18], refs[18:22], refs[22:]
    far_chip = lax.rem(lax.axis_index(axis) // CORES + 2, chips)
    layers = sources[0].shape[0]
    moves = []
    for i in range(9):
        src, dst = sources[i], results[i]
        if i < 3:
            for layer in range(layers):
                for who in range(chips - (i * per + layer * per // layers >= kept)):
                    for which in range(CORES):
                        at = (layer, lax.rem(far_chip + 1 + who, chips), which)
                        moves.append((src.at[at], dst.at[at], i // 2))
        else:
            for layer in range(layers):
                for half in range(2):
                    at = (layer, pl.ds(half * src.shape[1] // 2, src.shape[1] // 2))
                    moves.append((src.at[at], dst.at[at], 2 + i % 3 // 2))
    used = [0] * 4
    copies = []
    for src, dst, kind in moves:
        slot = used[kind] % COPY_SLOTS
        buffer = buffers[kind].at[slot]
        copies.append((pltpu.make_async_copy(src, buffer, in_sem.at[kind, slot]), pltpu.make_async_copy(buffer, dst, out_sem.at[kind, slot]), used[kind]))
        used[kind] += 1
    kinds = [kind for _, _, kind in moves]
    waited = set()

    def wait_for(i):
        if i not in waited:
            waited.add(i)
            copies[i][1].wait()

    for i in range(len(copies) + COPY_AHEAD):
        if i < len(copies):
            if copies[i][2] >= COPY_SLOTS:
                wait_for(next(j for j in range(i) if kinds[j] == kinds[i] and copies[j][2] == copies[i][2] - COPY_SLOTS))
            copies[i][0].start()
        if i >= COPY_AHEAD:
            copies[i - COPY_AHEAD][0].wait()
            copies[i - COPY_AHEAD][1].start()
    for i in range(len(copies)):
        wait_for(i)


def place_kernel(axis, chips, per, kept, partner, first, second, *refs):
    results, sem = refs[3:6], refs[6]
    me = lax.axis_index(axis)
    far_chip, core = lax.rem(me // CORES + 2, chips), lax.rem(me, CORES)
    which = 1 - core if partner else core
    quarters = per // 2
    for j in range(first.shape[0]):
        k, rest = (kept + j) // per, (kept + j) % per
        layer, q = rest // quarters, rest % quarters
        whole = results[k].at[layer, far_chip, which]
        where = whole.at[:, pl.ds(q * COLS, COLS)] if k < 2 else whole.at[q]
        pltpu.make_async_copy(first.at[j], where.at[A], sem.at[0]).start()
        pltpu.make_async_copy(second.at[j], where.at[B], sem.at[1]).start()
    pltpu.make_async_copy(first, first, sem.at[0]).wait()
    pltpu.make_async_copy(second, second, sem.at[1]).wait()


def solution(mesh):
    axis = "dp"
    chips = mesh.shape[axis] // CORES
    assert chips == 4

    def step(*arrays):
        def cut(x, rows, columns, split):
            lead = (x.shape[0],) + ((chips, CORES) if split else ())
            return x.reshape(*lead, *((rows, columns) if columns > COLS else (rows // ROWS, ROWS, columns)))

        shapes = [a.shape for a in arrays[6:9]]
        assert all(s[1] == ROWS for s in shapes[:2])
        per = shapes[0][0] * shapes[0][2] // COLS
        units = 3 * per
        g = [cut(a[0], s[1], s[2], True) for a, s in zip(arrays[:3], shapes, strict=True)]
        w = [cut(a, s[1], s[2], True) for a, s in zip(arrays[3:6], shapes, strict=True)]
        moments = [cut(a, s[1], s[2], False) for a, s in zip(arrays[6:], shapes + shapes, strict=True)]
        hbm, vmem = pl.BlockSpec(memory_space=pltpu.HBM), pl.BlockSpec(memory_space=pltpu.VMEM)
        results = [jax.ShapeDtypeStruct(x.shape, x.dtype) for x in (*w, *moments)]
        halves = jax.ShapeDtypeStruct((units - KEPT, HALF, COLS), jnp.bfloat16)
        *made, to_right, to_left = pl.pallas_call(
            functools.partial(kernel, axis, chips, per, units, KEPT),
            out_shape=[*results, halves, halves],
            in_specs=[hbm] * 12,
            out_specs=[hbm] * 11,
            scratch_shapes=[
                pltpu.VMEM((SLOTS, chips, ROWS, COLS), jnp.bfloat16),
                pltpu.VMEM((units, chips, ROWS, COLS), jnp.bfloat16),
                pltpu.VMEM((units, 2, ROWS, COLS), jnp.bfloat16),
                pltpu.VMEM((units, ROWS, COLS), jnp.bfloat16),
                pltpu.VMEM((SLOTS, ROWS, COLS), jnp.bfloat16),
                pltpu.VMEM((SLOTS, ROWS, COLS), jnp.float32),
                pltpu.VMEM((SLOTS, ROWS, COLS), jnp.float32),
                pltpu.SemaphoreType.DMA((SLOTS, 4)),
                pltpu.SemaphoreType.DMA((SLOTS, 2)),
                pltpu.SemaphoreType.DMA((units,)),
                pltpu.SemaphoreType.DMA((units,)),
                pltpu.SemaphoreType.DMA((units,)),
                pltpu.SemaphoreType.DMA((units,)),
                pltpu.SemaphoreType.DMA((units,)),
                pltpu.SemaphoreType.DMA((units,)),
                pltpu.SemaphoreType.DMA((SLOTS + 1, 2)),
                pltpu.SemaphoreType.DMA((13,)),
                pltpu.SemaphoreType.DMA((3,)),
                pltpu.SemaphoreType.DMA,
            ],
            compiler_params=pltpu.CompilerParams(collective_id=0, has_side_effects=True, vmem_limit_bytes=62 * 1024 * 1024),
        )(*g, *w, *moments)

        n = chips * CORES
        from_left = lax.ppermute(to_right, axis, [(i, (i + CORES) % n) for i in range(n)])
        from_right = lax.ppermute(to_left, axis, [(i, (i - CORES) % n) for i in range(n)])
        swap = [(i, i // CORES * CORES + 1 - i % CORES) for i in range(n)]
        result = pl.pallas_call(
            functools.partial(copy_kernel, axis, chips, per, KEPT),
            out_shape=results,
            in_specs=[hbm] * 9,
            out_specs=[hbm] * 9,
            scratch_shapes=[
                pltpu.VMEM((COPY_SLOTS, ROWS, 4 * COLS), jnp.bfloat16),
                pltpu.VMEM((COPY_SLOTS, 4, ROWS, COLS), jnp.bfloat16),
                pltpu.VMEM((COPY_SLOTS, HALF, 4 * COLS), jnp.float32),
                pltpu.VMEM((COPY_SLOTS, 2, ROWS, COLS), jnp.float32),
                pltpu.SemaphoreType.DMA((4, COPY_SLOTS)),
                pltpu.SemaphoreType.DMA((4, COPY_SLOTS)),
            ],
            compiler_params=pltpu.CompilerParams(has_side_effects=True, vmem_limit_bytes=52 * 1024 * 1024),
            cost_estimate=pl.CostEstimate(flops=10**9, bytes_accessed=2**27, transcendentals=0),
        )(*made)

        def place(result, first, second, partner):
            new = pl.pallas_call(
                functools.partial(place_kernel, axis, chips, per, KEPT, partner),
                out_shape=results[:3],
                in_specs=[vmem] * 2 + [hbm] * 3,
                out_specs=[hbm] * 3,
                input_output_aliases={2: 0, 3: 1, 4: 2},
                scratch_shapes=[pltpu.SemaphoreType.DMA((2,))],
                compiler_params=pltpu.CompilerParams(has_side_effects=True, vmem_limit_bytes=16 * 1024 * 1024),
                cost_estimate=pl.CostEstimate(flops=10**7, bytes_accessed=2**22, transcendentals=0),
            )(first, second, *result[:3])
            return [*new, *result[3:]]

        from_left, from_right, *result = lax.optimization_barrier((from_left, from_right, *result))
        others = lax.ppermute(from_left, axis, swap), lax.ppermute(from_right, axis, swap)
        result = place(result, from_left, from_right, False)
        result = place(result, *others, True)
        return tuple(x.reshape(a.shape) for x, a in zip(result, arrays[3:], strict=True))

    all_of, cut_of = P(None, None, None), P(None, "dp", None)
    return jax.shard_map(
        step,
        mesh=mesh,
        in_specs=(P(("rep", "dp"), None, None, None),) * 3 + (all_of,) * 3 + (cut_of,) * 6,
        out_specs=(P("rep", None, None),) * 3 + (P("rep", "dp", None),) * 6,
        check_vma=False,
    )
```
